32 devices in a mesh: expert: 4 (over x, core), row: 2 (over y), col: 4 (over z).
Axes of the slice: x: 2, y: 2, z: 4, core: 2. Of those that a mesh axis runs over, the one named last changes fastest.
Arguments:
- weights: bfloat16 [4, 4096, 7168], P('expert', 'row', 'col'), may hold values from -210 to 210
- inputs: bfloat16 [4, 1024, 4096], P('expert', ('row', 'col')), may hold values from -80 to 80
- cotangents: bfloat16 [4, 1024, 7168], P('expert', ('row', 'col')), may hold values from -150 to 150
- row_state: float32 [4, 4096], P('expert', 'row'), may hold values from 0.00089 to 0.91
- col_state: float32 [4, 7168], P('expert', 'col'), may hold values from 0.00089 to 0.91
Outputs:
- scaled_update: float32 [4, 4096, 7168], P('expert', 'row', 'col')
- new_row_state: float32 [4, 4096], P('expert', 'row')
- new_col_state: float32 [4, 7168], P('expert', 'col')
The draws below stay inside these ranges and needn't reach their ends.
All inputs are finite; a program needn't handle non-finite values.
Results may differ from the reference program's by a relative error of at most 0.0003.
Values may be sent and summed in bfloat16 or wider, within the bound.
A program may use at most 128 MiB of HBM per device.

```python
import math
import jax
import jax.numpy as jnp
from jax import lax

D = 4096
FF = 7168
STEP = 10
MATS = 4
TOK = 1024


def spread(key, array_shape, low_end, high_end):
    return jnp.exp(jax.random.uniform(key, array_shape, jnp.float32, math.log(low_end), math.log(high_end)))


def rising(length, factor):
    return factor ** (jnp.arange(length, dtype=jnp.float32) / length)


def draw_inputs(key, part):
    feature = spread(jax.random.fold_in(key, 11), (MATS, 1, D), 1.0, 10.0)
    values = jax.random.truncated_normal(jax.random.fold_in(key, 14), -6.0, 6.0, (MATS, TOK, D)) * feature * rising(D, 3.0)
    return (0.25 * values).astype(jnp.bfloat16)


def draw_cotangents(key, part):
    column_scale = spread(jax.random.fold_in(key, 21), (MATS, 1, FF), 1.0, 10.0) * rising(FF, 3.0)
    matrix_scale = rising(MATS, 3.0)[:, None, None]
    values = jax.random.truncated_normal(jax.random.fold_in(key, 24), -6.0, 6.0, (MATS, TOK, FF)) * column_scale * matrix_scale
    return (0.25 * values).astype(jnp.bfloat16)


def draw_weights(key, part):
    row_scale = spread(jax.random.fold_in(key, 31), (MATS, D, 1), 0.2, 2.0) * rising(D, 1.7)[:, None]
    column_scale = spread(jax.random.fold_in(key, 32), (MATS, 1, FF), 0.2, 2.0) * rising(FF, 1.7)
    matrix_level = spread(jax.random.fold_in(key, 36), (MATS, 1, 1), 0.3, 3.0)
    values = jax.random.truncated_normal(jax.random.fold_in(key, 35), -6.0, 6.0, (MATS, D, FF)) * row_scale * column_scale
    return (values * matrix_level).astype(jnp.bfloat16)


def draw_state(key, length):
    matrix_level = spread(jax.random.fold_in(key, 41), (MATS, 1), 0.003, 0.3)
    entry_scale = spread(jax.random.fold_in(key, 43), (MATS, length), 0.3, 3.0)
    return (matrix_level * entry_scale).astype(jnp.float32)


def draw_row_state(key, part):
    return draw_state(jax.random.fold_in(key, 51), D)


def draw_col_state(key, part):
    return draw_state(jax.random.fold_in(key, 52), FF)


def setup_inputs(seed: int = 0) -> dict:
    splits = jax.random.split(jax.random.key(seed), 6)
    weights = draw_weights(jax.random.fold_in(splits[5], 71), 0)
    inputs = draw_inputs(jax.random.fold_in(splits[5], 71), 0)
    cotangents = draw_cotangents(jax.random.fold_in(splits[5], 71), 0)
    row_state = draw_row_state(jax.random.fold_in(splits[5], 71), 0)
    col_state = draw_col_state(jax.random.fold_in(splits[5], 71), 0)
    return dict(weights=weights, inputs=inputs, cotangents=cotangents, row_state=row_state, col_state=col_state)


eps_square = 1e-30

def gradient(matrix_inputs, matrix_cotangents):
    return jnp.dot(matrix_inputs.astype(jnp.float32).T, matrix_cotangents.astype(jnp.float32), preferred_element_type=jnp.float32)

def reference(weights, inputs, cotangents, row_state, col_state):
    gradients = lax.map(lambda operand_pair: gradient(operand_pair[0], operand_pair[1]), (inputs, cotangents))
    squared_total = jnp.sum(gradients * gradients)
    clip_scale = 1.0 / jnp.maximum(1.0, jnp.sqrt(squared_total / (MATS * D * FF)))
    decay_rate = 1.0 - STEP ** (-0.8)

    def update_one(operands):
        matrix_weights, matrix_grad, old_rows, old_cols = operands
        clipped = clip_scale * matrix_grad
        squares = clipped * clipped + eps_square
        new_rows = decay_rate * old_rows + (1.0 - decay_rate) * lax.optimization_barrier(jnp.mean(squares, axis=1))
        new_cols = decay_rate * old_cols + (1.0 - decay_rate) * lax.optimization_barrier(jnp.mean(squares, axis=0))
        row_average = jnp.mean(new_rows)
        second = new_rows[:, None] * new_cols[None, :] / row_average
        update = clipped / jnp.sqrt(second)
        update_rms = jnp.sqrt(jnp.mean(update * update))
        update = update / jnp.maximum(1.0, update_rms)
        weights_wide = matrix_weights.astype(jnp.float32)
        weight_rms = jnp.sqrt(jnp.mean(weights_wide * weights_wide))
        return (weight_rms * update, new_rows, new_cols)
    scaled_update, new_rows, new_cols = lax.map(update_one, (weights, gradients, row_state, col_state))
    return (scaled_update, new_rows, new_cols)
```

```python
import functools

import jax
import jax.numpy as jnp
from jax import lax
from jax.experimental import pallas as pl
from jax.experimental.pallas import tpu as pltpu
from jax.sharding import PartitionSpec as P

STEP = 10
TILE = 256
CHUNKS = 4

eps_square = 1e-30


def kernel(
    E, Y, Z, total_entries, model_width, hidden_width,
    w_hbm, x_hbm, c_hbm, row_state, col_state,
    g_hbm, new_rows, new_cols, row_factor, col_factor,
    wbuf, xbuf, cbuf, grad, row_part, col_part, col_recv, row_recv, sq_recv, fin_recv,
    sx, rx, sxy, sc, rc, scy, local, out_sem,
    row_send_sem, row_recv_sem, col_send_sem, col_recv_sem, sq_send_sem, sq_recv_sem, fin_send_sem, fin_recv_sem,
):
    e, y, z = lax.axis_index("expert"), lax.axis_index("row"), lax.axis_index("col")
    other = 1 - y
    tokens = x_hbm.shape[0]
    rows, cols = grad.shape
    tiles = rows // TILE
    piece = tokens // CHUNKS
    decay_rate = 1.0 - STEP ** (-0.8)

    def dev(e_, y_, z_):
        return {"expert": e_, "row": y_, "col": z_}

    def remote(src, dst, send, recv, where):
        return pltpu.make_async_remote_copy(
            src_ref=src, dst_ref=dst, send_sem=send, recv_sem=recv,
            device_id=where, device_id_type=pl.DeviceIdType.MESH,
        )

    def group_peer(k):
        p = lax.rem(y * Z + z + k, Y * Z)
        return p // Z, lax.rem(p, Z)

    def expert_peer(k):
        p = lax.rem(e * Y + y + k, E * Y)
        return p // Y, lax.rem(p, Y)

    barrier = pltpu.get_barrier_semaphore()
    for k in range(1, Y * Z):
        yk, zk = group_peer(k)
        pl.semaphore_signal(barrier, inc=1, device_id=dev(e, yk, zk), device_id_type=pl.DeviceIdType.MESH)
    for k in range(1, E):
        for yk in range(Y):
            pl.semaphore_signal(
                barrier, inc=1, device_id=dev(lax.rem(e + k, E), yk, z), device_id_type=pl.DeviceIdType.MESH
            )

    own_x = pltpu.make_async_copy(
        x_hbm.at[:, pl.ds(pl.multiple_of(y * rows, TILE), rows)],
        xbuf.at[z, pl.ds(pl.multiple_of(y * tokens, tokens), tokens)], local.at[0])
    own_c = pltpu.make_async_copy(
        c_hbm.at[:, pl.ds(pl.multiple_of(z * cols, TILE), cols)],
        cbuf.at[z, pl.ds(pl.multiple_of(y * tokens, tokens), tokens)], local.at[1])
    weights_in = pltpu.make_async_copy(w_hbm, wbuf, local.at[2])
    own_x.start()
    own_c.start()
    weights_in.start()
    pl.semaphore_wait(barrier, Y * Z - 1 + (E - 1) * Y)

    def x_slot(s, q, h):
        return xbuf.at[s, pl.ds(pl.multiple_of(q * tokens + h * piece, piece), piece)]

    def x_own_src(half, h):
        return x_hbm.at[pl.ds(pl.multiple_of(h * piece, piece), piece),
                        pl.ds(pl.multiple_of(half * rows, TILE), rows)]

    def x_right(s, q, h, src):
        return remote(src, x_slot(s, q, h), sx.at[0, s, q, h], rx.at[s, q, h], dev(e, y, lax.rem(z + 1, Z)))

    def x_left(s, q, h, src):
        return remote(src, x_slot(s, q, h), sx.at[1, s, q, h], rx.at[s, q, h], dev(e, y, lax.rem(z + Z - 1, Z)))

    def x_cross(h):
        return remote(x_own_src(other, h), x_slot(z, y, h), sxy.at[h], rx.at[z, y, h], dev(e, other, z))

    def c_slot(s, q):
        return cbuf.at[s, pl.ds(pl.multiple_of(q * tokens, tokens), tokens)]

    def c_src(t):
        return c_hbm.at[:, pl.ds(pl.multiple_of(t * cols, TILE), cols)]

    def c_spread(k):
        t = lax.rem(z + k, Z)
        return remote(c_src(t), c_slot(z, y), sc.at[t], rc.at[z, y], dev(e, y, t))

    def c_cross(s, src):
        return remote(src, c_slot(s, y), scy.at[s], rc.at[s, y], dev(e, other, z))

    for h in range(CHUNKS):
        x_cross(h).start()
    for k in (2, 1, 3) if Z == 4 else range(1, Z):
        c_spread(k).start()
    c_cross(z, c_src(z)).start()

    def send_both(q, source):
        def step(h, carry):
            src = source(h)

            @pl.when(z < Z - 1)
            def _():
                x_right(z, q, h, src).start()

            @pl.when(z > 0)
            def _():
                x_left(z, q, h, src).start()
            return carry
        return step

    lax.fori_loop(0, CHUNKS, send_both(y, lambda h: x_own_src(y, h)), 0)

    def pass_cross(h, carry):
        slot = x_slot(z, other, h)
        x_right(z, other, h, slot).wait_recv()
        return send_both(other, lambda h: x_slot(z, other, h))(h, carry)

    weights_in.wait()

    def weight_tile(r, acc):
        block = wbuf[pl.ds(pl.multiple_of(r * 64, 64), 64), :].astype(jnp.float32)
        block = block * block
        part = block[0:8]
        for i in range(1, 8):
            part = part + block[8 * i:8 * i + 8]
        return acc + part

    weight_acc = lax.fori_loop(0, rows // 64, weight_tile, jnp.zeros((8, cols), jnp.float32))
    weight_sum = jnp.sum(weight_acc, axis=(0, 1), keepdims=True)

    lax.fori_loop(0, CHUNKS, pass_cross, 0)

    def each_side(d, act):
        @pl.when(z >= d)
        def _():
            act(z - d, True)

        @pl.when(z + d < Z)
        def _():
            act(z + d, False)

    def c_step(s, from_left):
        c_spread_recv = remote(c_slot(s, y), c_slot(s, y), sc.at[s], rc.at[s, y], dev(e, y, s))
        c_spread_recv.wait_recv()
        c_cross(s, c_slot(s, y)).start()

    def x_step(q):
        def act(s, from_left):
            def step(h, carry):
                slot = x_slot(s, q, h)
                x_right(s, q, h, slot).wait_recv()
                if from_left:
                    @pl.when(z < Z - 1)
                    def _():
                        x_right(s, q, h, slot).start()
                else:
                    @pl.when(z > 0)
                    def _():
                        x_left(s, q, h, slot).start()
                return carry
            lax.fori_loop(0, CHUNKS, step, 0)
        return act

    def wait_c_other(s):
        remote(c_slot(s, other), c_slot(s, other), scy.at[s], rc.at[s, other], dev(e, other, z)).wait_recv()

    def tile_ds(r):
        return pl.ds(pl.multiple_of(r * TILE, TILE), TILE)

    def compute(s, first):
        def step(r, carry):
            value = lax.dot_general(
                xbuf[s, :, tile_ds(r)], cbuf[s], (((0,), (0,)), ((), ())),
                preferred_element_type=jnp.float32)
            if first:
                grad[tile_ds(r), :] = value
            else:
                grad[tile_ds(r), :] += value
            return carry
        lax.fori_loop(0, tiles, step, 0)

    def compute_side(s, from_left):
        wait_c_other(s)
        compute(s, False)

    each_side(1, c_step)
    each_side(1, x_step(y))
    for d in range(2, Z):
        each_side(d, c_step)
    each_side(1, x_step(other))
    own_x.wait()
    own_c.wait()
    wait_c_other(z)
    compute(z, True)
    for d in range(1, Z):
        if d > 1:
            each_side(d, x_step(y))
            each_side(d, x_step(other))
        each_side(d, compute_side)

    def out_copy(r):
        return pltpu.make_async_copy(grad.at[tile_ds(r)], g_hbm.at[tile_ds(r)], out_sem.at[r])

    def fold_lanes(values):
        part = values[:, 0:128]
        for i in range(1, cols // 128):
            part = part + values[:, 128 * i:128 * i + 128]
        return jnp.sum(part.T, axis=0, keepdims=True)

    def stat_tile(r, acc):
        out_copy(r).start()
        block = grad[tile_ds(r), :]
        block = block * block
        row_part[pl.ds(r, 1), :] = fold_lanes(block)
        return acc + jnp.sum(block, axis=0, keepdims=True)

    col_part[...] = lax.fori_loop(0, tiles, stat_tile, jnp.zeros((1, cols), jnp.float32))

    def row_copy(k):
        return remote(row_part, row_recv.at[z], row_send_sem.at[k], row_recv_sem.at[z],
                      dev(e, y, lax.rem(z + k, Z)))

    col_copy = remote(col_part, col_recv, col_send_sem, col_recv_sem, dev(e, other, z))
    for k in range(1, Z):
        row_copy(k).start()
    col_copy.start()
    row_total = row_part[...]
    for k in range(1, Z):
        s = lax.rem(z + k, Z)
        remote(row_part, row_recv.at[s], row_send_sem.at[k], row_recv_sem.at[s], dev(e, y, s)).wait_recv()
        row_total = row_total + row_recv[s]

    me = e * Y + y
    half_total = jnp.sum(row_total, axis=(0, 1), keepdims=True)
    sq_recv[me] = jnp.broadcast_to(half_total, (8, 128))

    def sq_copy(k):
        ek, yk = expert_peer(k)
        return remote(sq_recv.at[me], sq_recv.at[me], sq_send_sem.at[k], sq_recv_sem.at[me], dev(ek, yk, z))

    for k in range(1, E * Y):
        sq_copy(k).start()
    col_copy.wait_recv()
    col_total = col_part[...] + col_recv[...]
    for k in range(1, E * Y):
        ek, yk = expert_peer(k)
        s = ek * Y + yk
        remote(sq_recv.at[s], sq_recv.at[s], sq_send_sem.at[k], sq_recv_sem.at[s], dev(ek, yk, z)).wait_recv()
    squared_total = sq_recv[0, 0:1, 0:1]
    for s in range(1, E * Y):
        squared_total = squared_total + sq_recv[s, 0:1, 0:1]
    clip = 1.0 / jnp.maximum(1.0, jnp.sqrt(squared_total / total_entries))
    clip_square = clip * clip
    rows_new = decay_rate * row_state[...] + (1.0 - decay_rate) * (clip_square * (row_total / hidden_width) + eps_square)
    cols_new = decay_rate * col_state[...] + (1.0 - decay_rate) * (clip_square * (col_total / model_width) + eps_square)
    new_rows[...] = rows_new
    new_cols[...] = cols_new
    row_part_inverse = 1.0 / rows_new
    row_factor[...] = row_part_inverse
    col_inverse = 1.0 / cols_new

    def update_tile(r, acc):
        block = grad[tile_ds(r), :]
        return acc + fold_lanes(block * block * col_inverse) * row_factor[pl.ds(r, 1), :]

    update_acc = lax.fori_loop(0, tiles, update_tile, jnp.zeros((1, TILE), jnp.float32))
    update_sum = jnp.sum(update_acc, axis=(0, 1), keepdims=True)
    rows_sum = jnp.sum(rows_new, axis=(0, 1), keepdims=True)

    mine = y * Z + z
    line = lax.broadcasted_iota(jnp.int32, (8, 128), 0)
    fin_recv[mine] = jnp.where(line == 0, update_sum, jnp.where(line == 1, weight_sum, rows_sum))

    def fin_copy(k):
        yk, zk = group_peer(k)
        return remote(fin_recv.at[mine], fin_recv.at[mine], fin_send_sem.at[k], fin_recv_sem.at[mine], dev(e, yk, zk))

    for k in range(1, Y * Z):
        fin_copy(k).start()

    for h in range(CHUNKS):
        x_cross(h).wait_send()
    for k in range(1, Z):
        c_spread(k).wait_send()
        row_copy(k).wait_send()
    col_copy.wait_send()
    for s in range(Z):
        c_cross(s, c_slot(s, y)).wait_send()
    for k in range(1, E * Y):
        sq_copy(k).wait_send()

    def sent(i, carry):
        s = i // (Y * CHUNKS)
        q = lax.rem(i // CHUNKS, Y)
        h = lax.rem(i, CHUNKS)

        @pl.when((s <= z) & (z < Z - 1))
        def _():
            x_right(s, q, h, x_slot(s, q, h)).wait_send()

        @pl.when((s >= z) & (z > 0))
        def _():
            x_left(s, q, h, x_slot(s, q, h)).wait_send()
        return carry

    lax.fori_loop(0, Z * Y * CHUNKS, sent, 0)

    for k in range(1, Y * Z):
        yk, zk = group_peer(k)
        s = yk * Z + zk
        remote(fin_recv.at[s], fin_recv.at[s], fin_send_sem.at[k], fin_recv_sem.at[s], dev(e, yk, zk)).wait_recv()
    total = fin_recv[0]
    for s in range(1, Y * Z):
        total = total + fin_recv[s]
    for k in range(1, Y * Z):
        fin_copy(k).wait_send()
    entries = model_width * hidden_width
    row_average = total[2:3, 0:1] / (Z * model_width)
    update_rms = jnp.sqrt(clip_square * row_average * total[0:1, 0:1] / entries)
    weight_rms = jnp.sqrt(total[1:2, 0:1] / entries)
    scalar = weight_rms / jnp.maximum(1.0, update_rms) * clip * jnp.sqrt(row_average)
    row_factor[...] = scalar * lax.rsqrt(rows_new)
    col_factor[...] = lax.rsqrt(cols_new)
    lax.fori_loop(0, tiles, lambda r, c: (out_copy(r).wait(), c)[1], 0)


def body(weights, inputs, cotangents, row_state, col_state):
    matrices, rows, cols = weights.shape
    tokens, model_width = inputs.shape[1:]
    hidden_width = cotangents.shape[2]
    E, Y, Z = lax.axis_size("expert"), lax.axis_size("row"), lax.axis_size("col")
    assert matrices == 1 and Y == 2
    tiles = rows // TILE
    f32 = jnp.float32
    vmem = pl.BlockSpec(memory_space=pltpu.VMEM)
    hbm = pl.BlockSpec(memory_space=pl.ANY)
    dma = pltpu.SemaphoreType.DMA
    grad, new_rows, new_cols, row_factor, col_factor = pl.pallas_call(
        functools.partial(
            kernel, E, Y, Z, float(matrices * E * model_width * hidden_width), float(model_width), float(hidden_width)
        ),
        out_shape=(
            jax.ShapeDtypeStruct((rows, cols), f32),
            jax.ShapeDtypeStruct((tiles, TILE), f32),
            jax.ShapeDtypeStruct((1, cols), f32),
            jax.ShapeDtypeStruct((tiles, TILE), f32),
            jax.ShapeDtypeStruct((1, cols), f32),
        ),
        in_specs=[hbm, hbm, hbm, vmem, vmem],
        out_specs=(hbm, vmem, vmem, vmem, vmem),
        scratch_shapes=[
            pltpu.VMEM((rows, cols), jnp.bfloat16),
            pltpu.VMEM((Z, Y * tokens, rows), jnp.bfloat16),
            pltpu.VMEM((Z, Y * tokens, cols), jnp.bfloat16),
            pltpu.VMEM((rows, cols), f32),
            pltpu.VMEM((tiles, TILE), f32),
            pltpu.VMEM((1, cols), f32),
            pltpu.VMEM((1, cols), f32),
            pltpu.VMEM((Z, tiles, TILE), f32),
            pltpu.VMEM((E * Y, 8, 128), f32),
            pltpu.VMEM((Y * Z, 8, 128), f32),
            dma((2, Z, Y, CHUNKS)),
            dma((Z, Y, CHUNKS)),
            dma((CHUNKS,)),
            dma((Z,)),
            dma((Z, Y)),
            dma((Z,)),
            dma((3,)),
            dma((tiles,)),
            dma((Z,)),
            dma((Z,)),
            dma,
            dma,
            dma((E * Y,)),
            dma((E * Y,)),
            dma((Y * Z,)),
            dma((Y * Z,)),
        ],
        compiler_params=pltpu.CompilerParams(
            collective_id=0, has_side_effects=True, vmem_limit_bytes=58 * 1024 * 1024
        ),
    )(
        weights.reshape(rows, cols), inputs.reshape(tokens, model_width), cotangents.reshape(tokens, hidden_width),
        row_state.reshape(tiles, TILE), col_state,
    )
    scaled = grad * row_factor.reshape(rows, 1) * col_factor
    return scaled[None], new_rows.reshape(1, rows), new_cols


def solution(mesh):
    in_specs = (
        P("expert", "row", "col"),
        P("expert", ("row", "col"), None),
        P("expert", ("row", "col"), None),
        P("expert", "row"),
        P("expert", "col"),
    )
    out_specs = (P("expert", "row", "col"), P("expert", "row"), P("expert", "col"))
    return jax.shard_map(body, mesh=mesh, in_specs=in_specs, out_specs=out_specs, check_vma=False)
```

```python
import functools

import jax
import jax.numpy as jnp
from jax import lax
from jax.experimental import pallas as pl
from jax.experimental.pallas import tpu as pltpu
from jax.sharding import PartitionSpec as P

STEP = 10
TILE = 256
CHUNKS = 4

eps_square = 1e-30


def kernel(
    E, Y, Z, total_entries, model_width, hidden_width,
    w_hbm, x_hbm, c_hbm, row_state, col_state,
    grad, new_rows, new_cols, row_factor, col_factor,
    wbuf, xbuf, cbuf, state, row_part, col_part, col_recv, row_recv, sq_recv, fin_recv,
    sx, rx, sxy, sc, rc, scy, local,
    row_send_sem, row_recv_sem, col_send_sem, col_recv_sem, sq_send_sem, sq_recv_sem, fin_send_sem, fin_recv_sem,
):
    e, y, z = lax.axis_index("expert"), lax.axis_index("row"), lax.axis_index("col")
    other = 1 - y
    tokens = x_hbm.shape[0]
    rows, cols = grad.shape
    tiles = rows // TILE
    piece = rows // CHUNKS
    chunk_tiles = tiles // CHUNKS
    decay_rate = 1.0 - STEP ** (-0.8)

    def dev(e_, y_, z_):
        return {"expert": e_, "row": y_, "col": z_}

    def remote(src, dst, send, recv, where):
        return pltpu.make_async_remote_copy(
            src_ref=src, dst_ref=dst, send_sem=send, recv_sem=recv,
            device_id=where, device_id_type=pl.DeviceIdType.MESH,
        )

    def group_peer(k):
        p = lax.rem(y * Z + z + k, Y * Z)
        return p // Z, lax.rem(p, Z)

    def expert_peer(k):
        p = lax.rem(e * Y + y + k, E * Y)
        return p // Y, lax.rem(p, Y)

    barrier = pltpu.get_barrier_semaphore()
    for k in range(1, Y * Z):
        yk, zk = group_peer(k)
        pl.semaphore_signal(barrier, inc=1, device_id=dev(e, yk, zk), device_id_type=pl.DeviceIdType.MESH)
    for k in range(1, E):
        for yk in range(Y):
            pl.semaphore_signal(
                barrier, inc=1, device_id=dev(lax.rem(e + k, E), yk, z), device_id_type=pl.DeviceIdType.MESH
            )

    own_x = pltpu.make_async_copy(
        x_hbm.at[:, pl.ds(pl.multiple_of(y * rows, TILE), rows)],
        xbuf.at[z, pl.ds(pl.multiple_of(y * tokens, tokens), tokens)], local.at[0])
    own_c = pltpu.make_async_copy(
        c_hbm.at[:, pl.ds(pl.multiple_of(z * cols, TILE), cols)],
        cbuf.at[z, pl.ds(pl.multiple_of(y * tokens, tokens), tokens)], local.at[1])
    weights_in = pltpu.make_async_copy(w_hbm, wbuf, local.at[2])
    own_x.start()
    own_c.start()
    weights_in.start()
    pl.semaphore_wait(barrier, Y * Z - 1 + (E - 1) * Y)

    def x_slot(s, q, h):
        return xbuf.at[s, pl.ds(pl.multiple_of(q * tokens, tokens), tokens), pl.ds(pl.multiple_of(h * piece, piece), piece)]

    def x_own_src(half, h):
        return x_hbm.at[:, pl.ds(pl.multiple_of(half * rows + h * piece, piece), piece)]

    def x_right(s, q, h, src):
        return remote(src, x_slot(s, q, h), sx.at[0, s, q, h], rx.at[s, q, h], dev(e, y, lax.rem(z + 1, Z)))

    def x_left(s, q, h, src):
        return remote(src, x_slot(s, q, h), sx.at[1, s, q, h], rx.at[s, q, h], dev(e, y, lax.rem(z + Z - 1, Z)))

    def x_cross(h):
        return remote(x_own_src(other, h), x_slot(z, y, h), sxy.at[h], rx.at[z, y, h], dev(e, other, z))

    def c_slot(s, q):
        return cbuf.at[s, pl.ds(pl.multiple_of(q * tokens, tokens), tokens)]

    def c_src(t):
        return c_hbm.at[:, pl.ds(pl.multiple_of(t * cols, TILE), cols)]

    def c_spread(k):
        t = lax.rem(z + k, Z)
        return remote(c_src(t), c_slot(z, y), sc.at[t], rc.at[z, y], dev(e, y, t))

    def c_cross(s, src):
        return remote(src, c_slot(s, y), scy.at[s], rc.at[s, y], dev(e, other, z))

    for h in range(CHUNKS):
        x_cross(h).start()
    for k in (2, 1, 3) if Z == 4 else range(1, Z):
        c_spread(k).start()
    c_cross(z, c_src(z)).start()

    def send_both(q, source):
        def step(h, carry):
            src = source(h)

            @pl.when(z < Z - 1)
            def _():
                x_right(z, q, h, src).start()

            @pl.when(z > 0)
            def _():
                x_left(z, q, h, src).start()
            return carry
        return step

    lax.fori_loop(0, CHUNKS, send_both(y, lambda h: x_own_src(y, h)), 0)

    def pass_cross(h, carry):
        slot = x_slot(z, other, h)
        x_right(z, other, h, slot).wait_recv()
        return send_both(other, lambda h: x_slot(z, other, h))(h, carry)

    weights_in.wait()

    def weight_tile(r, acc):
        block = wbuf[pl.ds(pl.multiple_of(r * 64, 64), 64), :].astype(jnp.float32)
        block = block * block
        part = block[0:8]
        for i in range(1, 8):
            part = part + block[8 * i:8 * i + 8]
        return acc + part

    weight_acc = lax.fori_loop(0, rows // 64, weight_tile, jnp.zeros((8, cols), jnp.float32))
    weight_sum = jnp.sum(weight_acc, axis=(0, 1), keepdims=True)

    lax.fori_loop(0, CHUNKS, pass_cross, 0)

    def each_side(d, act):
        @pl.when(z >= d)
        def _():
            act(z - d, True)

        @pl.when(z + d < Z)
        def _():
            act(z + d, False)

    def c_step(s, from_left):
        c_spread_recv = remote(c_slot(s, y), c_slot(s, y), sc.at[s], rc.at[s, y], dev(e, y, s))
        c_spread_recv.wait_recv()
        c_cross(s, c_slot(s, y)).start()

    def x_pass(s, q, h, from_left):
        slot = x_slot(s, q, h)
        x_right(s, q, h, slot).wait_recv()

        @pl.when(from_left & (z < Z - 1))
        def _():
            x_right(s, q, h, slot).start()

        @pl.when(jnp.logical_not(from_left) & (z > 0))
        def _():
            x_left(s, q, h, slot).start()

    def x_all(s, q, from_left):
        lax.fori_loop(0, CHUNKS, lambda h, carry: (x_pass(s, q, h, from_left), carry)[1], 0)

    def x_step(q):
        return lambda s, from_left: x_all(s, q, z >= s)

    def wait_c_other(s):
        remote(c_slot(s, other), c_slot(s, other), scy.at[s], rc.at[s, other], dev(e, other, z)).wait_recv()

    def tile_ds(r):
        return pl.ds(pl.multiple_of(r * TILE, TILE), TILE)

    def compute(s, first):
        def step(r, carry):
            value = lax.dot_general(
                xbuf[s, :, tile_ds(r)], cbuf[s], (((0,), (0,)), ((), ())),
                preferred_element_type=jnp.float32)
            if first:
                grad[tile_ds(r), :] = value
            else:
                grad[tile_ds(r), :] += value
            return carry
        lax.fori_loop(0, tiles, step, 0)

    def compute_side(s, from_left):
        wait_c_other(s)
        compute(s, False)

    from_left = 2 * z >= Z
    last = jnp.where(from_left, 0, Z - 1)

    def each_near(d, act):
        @pl.when((z >= d) & (z - d != last))
        def _():
            act(z - d, True)

        @pl.when((z + d < Z) & (z + d != last))
        def _():
            act(z + d, False)

    each_side(1, c_step)
    each_near(1, x_step(y))
    for d in range(2, Z):
        each_side(d, c_step)
    each_near(1, x_step(other))
    own_x.wait()
    own_c.wait()
    wait_c_other(z)
    compute(z, True)
    for d in range(1, Z - 1):
        if d > 1:
            each_near(d, x_step(y))
            each_near(d, x_step(other))
        each_near(d, compute_side)

    def fold_lanes(values):
        part = values[:, 0:128]
        for i in range(1, cols // 128):
            part = part + values[:, 128 * i:128 * i + 128]
        return jnp.sum(part.T, axis=0, keepdims=True)

    for r in range(tiles):
        state[r:r + 1, :] = row_state[:, r * TILE:(r + 1) * TILE]
    x_all(last, y, from_left)
    wait_c_other(last)

    def last_tile(r, acc):
        @pl.when(lax.rem(r, chunk_tiles) == 0)
        def _():
            x_pass(last, other, r // chunk_tiles, from_left)

        block = grad[tile_ds(r), :] + lax.dot_general(
            xbuf[last, :, tile_ds(r)], cbuf[last], (((0,), (0,)), ((), ())),
            preferred_element_type=jnp.float32)
        grad[tile_ds(r), :] = block
        block = block * block
        row_part[pl.ds(r, 1), :] = fold_lanes(block)
        part = block[0:8]
        for i in range(1, TILE // 8):
            part = part + block[8 * i:8 * i + 8]
        return acc + part

    col_acc = lax.fori_loop(0, tiles, last_tile, jnp.zeros((8, cols), jnp.float32))
    col_part[...] = jnp.sum(col_acc, axis=0, keepdims=True)

    def row_copy(k):
        return remote(row_part, row_recv.at[z], row_send_sem.at[k], row_recv_sem.at[z],
                      dev(e, y, lax.rem(z + k, Z)))

    col_copy = remote(col_part, col_recv, col_send_sem, col_recv_sem, dev(e, other, z))
    for k in range(1, Z):
        row_copy(k).start()
    col_copy.start()
    row_total = row_part[...]
    for k in range(1, Z):
        s = lax.rem(z + k, Z)
        remote(row_part, row_recv.at[s], row_send_sem.at[k], row_recv_sem.at[s], dev(e, y, s)).wait_recv()
        row_total = row_total + row_recv[s]

    me = e * Y + y
    half_total = jnp.sum(row_total, axis=(0, 1), keepdims=True)
    sq_recv[me] = jnp.broadcast_to(half_total, (8, 128))

    def sq_copy(k):
        ek, yk = expert_peer(k)
        return remote(sq_recv.at[me], sq_recv.at[me], sq_send_sem.at[k], sq_recv_sem.at[me], dev(ek, yk, z))

    for k in range(1, E * Y):
        sq_copy(k).start()
    col_copy.wait_recv()
    col_total = col_part[...] + col_recv[...]
    for k in range(1, E * Y):
        ek, yk = expert_peer(k)
        s = ek * Y + yk
        remote(sq_recv.at[s], sq_recv.at[s], sq_send_sem.at[k], sq_recv_sem.at[s], dev(ek, yk, z)).wait_recv()
    squared_total = sq_recv[0, 0:1, 0:1]
    for s in range(1, E * Y):
        squared_total = squared_total + sq_recv[s, 0:1, 0:1]
    clip = 1.0 / jnp.maximum(1.0, jnp.sqrt(squared_total / total_entries))
    clip_square = clip * clip
    rows_new = decay_rate * state[...] + (1.0 - decay_rate) * (clip_square * (row_total / hidden_width) + eps_square)
    cols_new = decay_rate * col_state[...] + (1.0 - decay_rate) * (clip_square * (col_total / model_width) + eps_square)
    new_rows[...] = rows_new
    new_cols[...] = cols_new
    row_part_inverse = 1.0 / rows_new
    row_factor[...] = row_part_inverse
    col_inverse = 1.0 / cols_new

    def update_tile(r, acc):
        block = grad[tile_ds(r), :]
        return acc + fold_lanes(block * block * col_inverse) * row_factor[pl.ds(r, 1), :]

    update_acc = lax.fori_loop(0, tiles, update_tile, jnp.zeros((1, TILE), jnp.float32))
    update_sum = jnp.sum(update_acc, axis=(0, 1), keepdims=True)
    rows_sum = jnp.sum(rows_new, axis=(0, 1), keepdims=True)

    mine = y * Z + z
    line = lax.broadcasted_iota(jnp.int32, (8, 128), 0)
    fin_recv[mine] = jnp.where(line == 0, update_sum, jnp.where(line == 1, weight_sum, rows_sum))

    def fin_copy(k):
        yk, zk = group_peer(k)
        return remote(fin_recv.at[mine], fin_recv.at[mine], fin_send_sem.at[k], fin_recv_sem.at[mine], dev(e, yk, zk))

    for k in range(1, Y * Z):
        fin_copy(k).start()

    for h in range(CHUNKS):
        x_cross(h).wait_send()
    for k in range(1, Z):
        c_spread(k).wait_send()
        row_copy(k).wait_send()
    col_copy.wait_send()
    for s in range(Z):
        c_cross(s, c_slot(s, y)).wait_send()
    for k in range(1, E * Y):
        sq_copy(k).wait_send()

    def sent(i, carry):
        s = i // (Y * CHUNKS)
        q = lax.rem(i // CHUNKS, Y)
        h = lax.rem(i, CHUNKS)

        @pl.when((s <= z) & (z < Z - 1))
        def _():
            x_right(s, q, h, x_slot(s, q, h)).wait_send()

        @pl.when((s >= z) & (z > 0))
        def _():
            x_left(s, q, h, x_slot(s, q, h)).wait_send()
        return carry

    lax.fori_loop(0, Z * Y * CHUNKS, sent, 0)

    for k in range(1, Y * Z):
        yk, zk = group_peer(k)
        s = yk * Z + zk
        remote(fin_recv.at[s], fin_recv.at[s], fin_send_sem.at[k], fin_recv_sem.at[s], dev(e, yk, zk)).wait_recv()
    total = fin_recv[0]
    for s in range(1, Y * Z):
        total = total + fin_recv[s]
    for k in range(1, Y * Z):
        fin_copy(k).wait_send()
    entries = model_width * hidden_width
    row_average = total[2:3, 0:1] / (Z * model_width)
    update_rms = jnp.sqrt(clip_square * row_average * total[0:1, 0:1] / entries)
    weight_rms = jnp.sqrt(total[1:2, 0:1] / entries)
    scalar = weight_rms / jnp.maximum(1.0, update_rms) * clip * jnp.sqrt(row_average)
    row_factor[...] = scalar * lax.rsqrt(rows_new)
    col_factor[...] = lax.rsqrt(cols_new)


def scale_kernel(grad, rows_in, cols_in, row_factor, col_factor, out, rows_out, cols_out, held, sems):
    rows, cols = grad.shape
    tiles = rows // TILE

    def copy(r):
        span = pl.ds(pl.multiple_of(r * TILE, TILE), TILE)
        return pltpu.make_async_copy(held.at[span], out.at[span], sems.at[r])

    def tile(r, carry):
        span = pl.ds(pl.multiple_of(r * TILE, TILE), TILE)
        factor = jnp.broadcast_to(row_factor[pl.ds(r, 1), :], (128, TILE)).T
        for i in range(cols // 128):
            lanes = slice(128 * i, 128 * i + 128)
            held[span, lanes] = grad[span, lanes] * factor * col_factor[:, lanes]
        copy(r).start()
        return carry

    lax.fori_loop(0, tiles, tile, 0)
    for r in range(tiles):
        rows_out[:, r * TILE:(r + 1) * TILE] = rows_in[r:r + 1, :]
    cols_out[...] = cols_in[...]
    lax.fori_loop(0, tiles, lambda r, c: (copy(r).wait(), c)[1], 0)


def body(weights, inputs, cotangents, row_state, col_state):
    matrices, rows, cols = weights.shape
    tokens, model_width = inputs.shape[1:]
    hidden_width = cotangents.shape[2]
    E, Y, Z = lax.axis_size("expert"), lax.axis_size("row"), lax.axis_size("col")
    assert matrices == 1 and Y == 2
    tiles = rows // TILE
    f32 = jnp.float32
    vmem = pl.BlockSpec(memory_space=pltpu.VMEM)
    hbm = pl.BlockSpec(memory_space=pl.ANY)
    dma = pltpu.SemaphoreType.DMA
    grad, new_rows, new_cols, row_factor, col_factor = pl.pallas_call(
        functools.partial(
            kernel, E, Y, Z, float(matrices * E * model_width * hidden_width), float(model_width), float(hidden_width)
        ),
        out_shape=(
            pltpu.VMEM((rows, cols), f32),
            pltpu.VMEM((tiles, TILE), f32),
            pltpu.VMEM((1, cols), f32),
            pltpu.VMEM((tiles, TILE), f32),
            pltpu.VMEM((1, cols), f32),
        ),
        in_specs=[hbm, hbm, hbm, vmem, vmem],
        out_specs=(vmem, vmem, vmem, vmem, vmem),
        scratch_shapes=[
            pltpu.VMEM((rows, cols), jnp.bfloat16),
            pltpu.VMEM((Z, Y * tokens, rows), jnp.bfloat16),
            pltpu.VMEM((Z, Y * tokens, cols), jnp.bfloat16),
            pltpu.VMEM((tiles, TILE), f32),
            pltpu.VMEM((tiles, TILE), f32),
            pltpu.VMEM((1, cols), f32),
            pltpu.VMEM((1, cols), f32),
            pltpu.VMEM((Z, tiles, TILE), f32),
            pltpu.VMEM((E * Y, 8, 128), f32),
            pltpu.VMEM((Y * Z, 8, 128), f32),
            dma((2, Z, Y, CHUNKS)),
            dma((Z, Y, CHUNKS)),
            dma((CHUNKS,)),
            dma((Z,)),
            dma((Z, Y)),
            dma((Z,)),
            dma((3,)),
            dma((Z,)),
            dma((Z,)),
            dma,
            dma,
            dma((E * Y,)),
            dma((E * Y,)),
            dma((Y * Z,)),
            dma((Y * Z,)),
        ],
        compiler_params=pltpu.CompilerParams(
            collective_id=0, has_side_effects=True, vmem_limit_bytes=44 * 1024 * 1024
        ),
    )(
        weights.reshape(rows, cols), inputs.reshape(tokens, model_width), cotangents.reshape(tokens, hidden_width),
        row_state, col_state,
    )
    scaled, new_rows, new_cols = pl.pallas_call(
        scale_kernel,
        out_shape=(
            jax.ShapeDtypeStruct((rows, cols), f32),
            jax.ShapeDtypeStruct((1, rows), f32),
            jax.ShapeDtypeStruct((1, cols), f32),
        ),
        in_specs=[vmem] * 5,
        out_specs=(hbm, vmem, vmem),
        scratch_shapes=[pltpu.VMEM((rows, cols), f32), dma((tiles,))],
        compiler_params=pltpu.CompilerParams(vmem_limit_bytes=17 * 1024 * 1024),
    )(grad, new_rows, new_cols, row_factor, col_factor)
    return scaled[None], new_rows, new_cols


def solution(mesh):
    in_specs = (
        P("expert", "row", "col"),
        P("expert", ("row", "col"), None),
        P("expert", ("row", "col"), None),
        P("expert", "row"),
        P("expert", "col"),
    )
    out_specs = (P("expert", "row", "col"), P("expert", "row"), P("expert", "col"))
    return jax.shard_map(body, mesh=mesh, in_specs=in_specs, out_specs=out_specs, check_vma=False)
```

```python
import functools

import jax
import jax.numpy as jnp
from jax import lax
from jax.experimental import pallas as pl
from jax.experimental.pallas import tpu as pltpu
from jax.sharding import PartitionSpec as P

STEP = 10
TILE = 256
CHUNKS = 4

eps_square = 1e-30


def kernel(
    E, Y, Z, total_entries, model_width, hidden_width,
    w_hbm, x_hbm, c_hbm, row_state, col_state,
    grad, new_rows, new_cols, row_factor, col_factor,
    wbuf, xbuf, cbuf, state, row_part, col_part, col_recv, row_recv, sq_recv, fin_recv,
    sx, rx, sxy, sc, rc, scy, local,
    row_send_sem, row_recv_sem, col_send_sem, col_recv_sem, sq_send_sem, sq_recv_sem, fin_send_sem, fin_recv_sem,
):
    e, y, z = lax.axis_index("expert"), lax.axis_index("row"), lax.axis_index("col")
    other = 1 - y
    tokens = x_hbm.shape[0]
    rows, cols = grad.shape
    tiles = rows // TILE
    piece = rows // CHUNKS
    chunk_tiles = tiles // CHUNKS
    decay_rate = 1.0 - STEP ** (-0.8)

    def dev(e_, y_, z_):
        return {"expert": e_, "row": y_, "col": z_}

    def remote(src, dst, send, recv, where):
        return pltpu.make_async_remote_copy(
            src_ref=src, dst_ref=dst, send_sem=send, recv_sem=recv,
            device_id=where, device_id_type=pl.DeviceIdType.MESH,
        )

    def group_peer(k):
        p = lax.rem(y * Z + z + k, Y * Z)
        return p // Z, lax.rem(p, Z)

    everyone = E * Y * Z
    me = (e * Y + y) * Z + z

    def any_peer(k):
        p = lax.rem(me + k, everyone)
        return p, dev(p // (Y * Z), lax.rem(p // Z, Y), lax.rem(p, Z))

    barrier = pltpu.get_barrier_semaphore()

    def greet(k, carry):
        pl.semaphore_signal(barrier, inc=1, device_id=any_peer(k)[1], device_id_type=pl.DeviceIdType.MESH)
        return carry

    lax.fori_loop(1, everyone, greet, 0)

    own_x = pltpu.make_async_copy(
        x_hbm.at[:, pl.ds(pl.multiple_of(y * rows, TILE), rows)],
        xbuf.at[z, pl.ds(pl.multiple_of(y * tokens, tokens), tokens)], local.at[0])
    own_c = pltpu.make_async_copy(
        c_hbm.at[:, pl.ds(pl.multiple_of(z * cols, TILE), cols)],
        cbuf.at[z, pl.ds(pl.multiple_of(y * tokens, tokens), tokens)], local.at[1])
    weights_in = pltpu.make_async_copy(w_hbm, wbuf, local.at[2])
    own_x.start()
    own_c.start()
    weights_in.start()
    pl.semaphore_wait(barrier, everyone - 1)

    def x_slot(s, q, h):
        return xbuf.at[s, pl.ds(pl.multiple_of(q * tokens, tokens), tokens), pl.ds(pl.multiple_of(h * piece, piece), piece)]

    def x_own_src(half, h):
        return x_hbm.at[:, pl.ds(pl.multiple_of(half * rows + h * piece, piece), piece)]

    def x_right(s, q, h, src):
        return remote(src, x_slot(s, q, h), sx.at[0, s, q, h], rx.at[s, q, h], dev(e, y, lax.rem(z + 1, Z)))

    def x_left(s, q, h, src):
        return remote(src, x_slot(s, q, h), sx.at[1, s, q, h], rx.at[s, q, h], dev(e, y, lax.rem(z + Z - 1, Z)))

    def x_cross(h):
        return remote(x_own_src(other, h), x_slot(z, y, h), sxy.at[h], rx.at[z, y, h], dev(e, other, z))

    def c_slot(s, q):
        return cbuf.at[s, pl.ds(pl.multiple_of(q * tokens, tokens), tokens)]

    def c_src(t):
        return c_hbm.at[:, pl.ds(pl.multiple_of(t * cols, TILE), cols)]

    def c_spread(k):
        t = lax.rem(z + k, Z)
        return remote(c_src(t), c_slot(z, y), sc.at[t], rc.at[z, y], dev(e, y, t))

    def c_cross(s, src):
        return remote(src, c_slot(s, y), scy.at[s], rc.at[s, y], dev(e, other, z))

    for h in range(CHUNKS):
        x_cross(h).start()
    for k in (2, 1, 3) if Z == 4 else range(1, Z):
        c_spread(k).start()
    c_cross(z, c_src(z)).start()

    def send_both(q, source):
        def step(h, carry):
            src = source(h)

            @pl.when(z < Z - 1)
            def _():
                x_right(z, q, h, src).start()

            @pl.when(z > 0)
            def _():
                x_left(z, q, h, src).start()
            return carry
        return step

    lax.fori_loop(0, CHUNKS, send_both(y, lambda h: x_own_src(y, h)), 0)

    def pass_cross(h, carry):
        slot = x_slot(z, other, h)
        x_right(z, other, h, slot).wait_recv()
        return send_both(other, lambda h: x_slot(z, other, h))(h, carry)

    weights_in.wait()

    def weight_tile(r, acc):
        block = wbuf[pl.ds(pl.multiple_of(r * 64, 64), 64), :].astype(jnp.float32)
        block = block * block
        part = block[0:8]
        for i in range(1, 8):
            part = part + block[8 * i:8 * i + 8]
        return acc + part

    weight_acc = lax.fori_loop(0, rows // 64, weight_tile, jnp.zeros((8, cols), jnp.float32))
    weight_sum = jnp.sum(weight_acc, axis=(0, 1), keepdims=True)

    lax.fori_loop(0, CHUNKS, pass_cross, 0)

    def each_side(d, act):
        @pl.when(z >= d)
        def _():
            act(z - d, True)

        @pl.when(z + d < Z)
        def _():
            act(z + d, False)

    def c_step(s, from_left):
        c_spread_recv = remote(c_slot(s, y), c_slot(s, y), sc.at[s], rc.at[s, y], dev(e, y, s))
        c_spread_recv.wait_recv()
        c_cross(s, c_slot(s, y)).start()

    def x_pass(s, q, h, from_left):
        slot = x_slot(s, q, h)
        x_right(s, q, h, slot).wait_recv()

        @pl.when(from_left & (z < Z - 1))
        def _():
            x_right(s, q, h, slot).start()

        @pl.when(jnp.logical_not(from_left) & (z > 0))
        def _():
            x_left(s, q, h, slot).start()

    def x_all(s, q, from_left):
        lax.fori_loop(0, CHUNKS, lambda h, carry: (x_pass(s, q, h, from_left), carry)[1], 0)

    def x_step(q):
        return lambda s, from_left: x_all(s, q, z >= s)

    def wait_c_other(s):
        remote(c_slot(s, other), c_slot(s, other), scy.at[s], rc.at[s, other], dev(e, other, z)).wait_recv()

    def tile_ds(r):
        return pl.ds(pl.multiple_of(r * TILE, TILE), TILE)

    def compute(s, first):
        def step(r, carry):
            value = lax.dot_general(
                xbuf[s, :, tile_ds(r)], cbuf[s], (((0,), (0,)), ((), ())),
                preferred_element_type=jnp.float32)
            if first:
                grad[tile_ds(r), :] = value
            else:
                grad[tile_ds(r), :] += value
            return carry
        lax.fori_loop(0, tiles, step, 0)

    def compute_side(s, from_left):
        wait_c_other(s)
        compute(s, False)

    from_left = 2 * z >= Z
    last = jnp.where(from_left, 0, Z - 1)

    def each_near(d, act):
        @pl.when((z >= d) & (z - d != last))
        def _():
            act(z - d, True)

        @pl.when((z + d < Z) & (z + d != last))
        def _():
            act(z + d, False)

    each_side(1, c_step)
    each_near(1, x_step(y))
    for d in range(2, Z):
        each_side(d, c_step)
    each_near(1, x_step(other))
    own_x.wait()
    own_c.wait()
    wait_c_other(z)
    compute(z, True)
    for d in range(1, Z - 1):
        if d > 1:
            each_near(d, x_step(y))
            each_near(d, x_step(other))
        each_near(d, compute_side)

    def fold_lanes(values):
        part = values[:, 0:128]
        for i in range(1, cols // 128):
            part = part + values[:, 128 * i:128 * i + 128]
        return jnp.sum(part.T, axis=0, keepdims=True)

    for r in range(tiles):
        state[r:r + 1, :] = row_state[:, r * TILE:(r + 1) * TILE]
    x_all(last, y, from_left)
    wait_c_other(last)

    def last_tile(r, acc):
        @pl.when(lax.rem(r, chunk_tiles) == 0)
        def _():
            x_pass(last, other, r // chunk_tiles, from_left)

        block = grad[tile_ds(r), :] + lax.dot_general(
            xbuf[last, :, tile_ds(r)], cbuf[last], (((0,), (0,)), ((), ())),
            preferred_element_type=jnp.float32)
        grad[tile_ds(r), :] = block
        block = block * block
        row_part[pl.ds(r, 1), :] = fold_lanes(block)
        part = block[0:8]
        for i in range(1, TILE // 8):
            part = part + block[8 * i:8 * i + 8]
        return acc + part

    col_acc = lax.fori_loop(0, tiles, last_tile, jnp.zeros((8, cols), jnp.float32))
    col_part[...] = jnp.sum(col_acc, axis=0, keepdims=True)

    def row_copy(k):
        return remote(row_part, row_recv.at[z], row_send_sem.at[k], row_recv_sem.at[z],
                      dev(e, y, lax.rem(z + k, Z)))

    col_copy = remote(col_part, col_recv, col_send_sem, col_recv_sem, dev(e, other, z))
    own_total = jnp.sum(row_part[...], axis=(0, 1), keepdims=True)
    sq_recv[me] = jnp.broadcast_to(own_total, (1, 128))

    def sq_copy(k):
        return remote(sq_recv.at[me], sq_recv.at[me], sq_send_sem.at[k], sq_recv_sem.at[me], any_peer(k)[1])

    for k in range(1, Z):
        row_copy(k).start()
    col_copy.start()
    lax.fori_loop(1, everyone, lambda k, carry: (sq_copy(k).start(), carry)[1], 0)
    row_total = row_part[...]
    for k in range(1, Z):
        s = lax.rem(z + k, Z)
        remote(row_part, row_recv.at[s], row_send_sem.at[k], row_recv_sem.at[s], dev(e, y, s)).wait_recv()
        row_total = row_total + row_recv[s]

    col_copy.wait_recv()
    col_total = col_part[...] + col_recv[...]

    def sq_arrived(k, carry):
        p, where = any_peer(k)
        remote(sq_recv.at[p], sq_recv.at[p], sq_send_sem.at[k], sq_recv_sem.at[p], where).wait_recv()
        return carry

    lax.fori_loop(1, everyone, sq_arrived, 0)
    squared_total = jnp.sum(sq_recv[...], axis=0)[:, 0:1]
    clip = 1.0 / jnp.maximum(1.0, jnp.sqrt(squared_total / total_entries))
    clip_square = clip * clip
    rows_new = decay_rate * state[...] + (1.0 - decay_rate) * (clip_square * (row_total / hidden_width) + eps_square)
    cols_new = decay_rate * col_state[...] + (1.0 - decay_rate) * (clip_square * (col_total / model_width) + eps_square)
    new_rows[...] = rows_new
    new_cols[...] = cols_new
    row_part_inverse = 1.0 / rows_new
    row_factor[...] = row_part_inverse
    col_inverse = 1.0 / cols_new

    def update_tile(r, acc):
        block = grad[tile_ds(r), :]
        return acc + fold_lanes(block * block * col_inverse) * row_factor[pl.ds(r, 1), :]

    update_acc = lax.fori_loop(0, tiles, update_tile, jnp.zeros((1, TILE), jnp.float32))
    update_sum = jnp.sum(update_acc, axis=(0, 1), keepdims=True)
    rows_sum = jnp.sum(rows_new, axis=(0, 1), keepdims=True)

    mine = y * Z + z
    line = lax.broadcasted_iota(jnp.int32, (8, 128), 0)
    fin_recv[mine] = jnp.where(line == 0, update_sum, jnp.where(line == 1, weight_sum, rows_sum))

    def fin_copy(k):
        yk, zk = group_peer(k)
        return remote(fin_recv.at[mine], fin_recv.at[mine], fin_send_sem.at[k], fin_recv_sem.at[mine], dev(e, yk, zk))

    for k in range(1, Y * Z):
        fin_copy(k).start()

    for h in range(CHUNKS):
        x_cross(h).wait_send()
    for k in range(1, Z):
        c_spread(k).wait_send()
        row_copy(k).wait_send()
    col_copy.wait_send()
    for s in range(Z):
        c_cross(s, c_slot(s, y)).wait_send()
    lax.fori_loop(1, everyone, lambda k, carry: (sq_copy(k).wait_send(), carry)[1], 0)

    def sent(i, carry):
        s = i // (Y * CHUNKS)
        q = lax.rem(i // CHUNKS, Y)
        h = lax.rem(i, CHUNKS)

        @pl.when((s <= z) & (z < Z - 1))
        def _():
            x_right(s, q, h, x_slot(s, q, h)).wait_send()

        @pl.when((s >= z) & (z > 0))
        def _():
            x_left(s, q, h, x_slot(s, q, h)).wait_send()
        return carry

    lax.fori_loop(0, Z * Y * CHUNKS, sent, 0)

    for k in range(1, Y * Z):
        yk, zk = group_peer(k)
        s = yk * Z + zk
        remote(fin_recv.at[s], fin_recv.at[s], fin_send_sem.at[k], fin_recv_sem.at[s], dev(e, yk, zk)).wait_recv()
    total = fin_recv[0]
    for s in range(1, Y * Z):
        total = total + fin_recv[s]
    for k in range(1, Y * Z):
        fin_copy(k).wait_send()
    entries = model_width * hidden_width
    row_average = total[2:3, 0:1] / (Z * model_width)
    update_rms = jnp.sqrt(clip_square * row_average * total[0:1, 0:1] / entries)
    weight_rms = jnp.sqrt(total[1:2, 0:1] / entries)
    scalar = weight_rms / jnp.maximum(1.0, update_rms) * clip * jnp.sqrt(row_average)
    row_factor[...] = scalar * lax.rsqrt(rows_new)
    col_factor[...] = lax.rsqrt(cols_new)


def scale_kernel(grad, rows_in, cols_in, row_factor, col_factor, out, rows_out, cols_out, held, sems):
    rows, cols = grad.shape
    tiles = rows // TILE

    def copy(r):
        span = pl.ds(pl.multiple_of(r * TILE, TILE), TILE)
        return pltpu.make_async_copy(held.at[span], out.at[span], sems.at[r])

    def tile(r, carry):
        span = pl.ds(pl.multiple_of(r * TILE, TILE), TILE)
        factor = jnp.broadcast_to(row_factor[pl.ds(r, 1), :], (128, TILE)).T
        for i in range(cols // 128):
            lanes = slice(128 * i, 128 * i + 128)
            held[span, lanes] = grad[span, lanes] * factor * col_factor[:, lanes]
        copy(r).start()
        return carry

    lax.fori_loop(0, tiles, tile, 0)
    for r in range(tiles):
        rows_out[:, r * TILE:(r + 1) * TILE] = rows_in[r:r + 1, :]
    cols_out[...] = cols_in[...]
    lax.fori_loop(0, tiles, lambda r, c: (copy(r).wait(), c)[1], 0)


def body(weights, inputs, cotangents, row_state, col_state):
    matrices, rows, cols = weights.shape
    tokens, model_width = inputs.shape[1:]
    hidden_width = cotangents.shape[2]
    E, Y, Z = lax.axis_size("expert"), lax.axis_size("row"), lax.axis_size("col")
    assert matrices == 1 and Y == 2
    tiles = rows // TILE
    f32 = jnp.float32
    vmem = pl.BlockSpec(memory_space=pltpu.VMEM)
    hbm = pl.BlockSpec(memory_space=pl.ANY)
    dma = pltpu.SemaphoreType.DMA
    grad, new_rows, new_cols, row_factor, col_factor = pl.pallas_call(
        functools.partial(
            kernel, E, Y, Z, float(matrices * E * model_width * hidden_width), float(model_width), float(hidden_width)
        ),
        out_shape=(
            pltpu.VMEM((rows, cols), f32),
            pltpu.VMEM((tiles, TILE), f32),
            pltpu.VMEM((1, cols), f32),
            pltpu.VMEM((tiles, TILE), f32),
            pltpu.VMEM((1, cols), f32),
        ),
        in_specs=[hbm, hbm, hbm, vmem, vmem],
        out_specs=(vmem, vmem, vmem, vmem, vmem),
        scratch_shapes=[
            pltpu.VMEM((rows, cols), jnp.bfloat16),
            pltpu.VMEM((Z, Y * tokens, rows), jnp.bfloat16),
            pltpu.VMEM((Z, Y * tokens, cols), jnp.bfloat16),
            pltpu.VMEM((tiles, TILE), f32),
            pltpu.VMEM((tiles, TILE), f32),
            pltpu.VMEM((1, cols), f32),
            pltpu.VMEM((1, cols), f32),
            pltpu.VMEM((Z, tiles, TILE), f32),
            pltpu.VMEM((E * Y * Z, 1, 128), f32),
            pltpu.VMEM((Y * Z, 8, 128), f32),
            dma((2, Z, Y, CHUNKS)),
            dma((Z, Y, CHUNKS)),
            dma((CHUNKS,)),
            dma((Z,)),
            dma((Z, Y)),
            dma((Z,)),
            dma((3,)),
            dma((Z,)),
            dma((Z,)),
            dma,
            dma,
            dma((E * Y * Z,)),
            dma((E * Y * Z,)),
            dma((Y * Z,)),
            dma((Y * Z,)),
        ],
        compiler_params=pltpu.CompilerParams(
            collective_id=0, has_side_effects=True, vmem_limit_bytes=44 * 1024 * 1024
        ),
    )(
        weights.reshape(rows, cols), inputs.reshape(tokens, model_width), cotangents.reshape(tokens, hidden_width),
        row_state, col_state,
    )
    scaled, new_rows, new_cols = pl.pallas_call(
        scale_kernel,
        out_shape=(
            jax.ShapeDtypeStruct((rows, cols), f32),
            jax.ShapeDtypeStruct((1, rows), f32),
            jax.ShapeDtypeStruct((1, cols), f32),
        ),
        in_specs=[vmem] * 5,
        out_specs=(hbm, vmem, vmem),
        scratch_shapes=[pltpu.VMEM((rows, cols), f32), dma((tiles,))],
        compiler_params=pltpu.CompilerParams(vmem_limit_bytes=17 * 1024 * 1024),
    )(grad, new_rows, new_cols, row_factor, col_factor)
    return scaled[None], new_rows, new_cols


def solution(mesh):
    in_specs = (
        P("expert", "row", "col"),
        P("expert", ("row", "col"), None),
        P("expert", ("row", "col"), None),
        P("expert", "row"),
        P("expert", "col"),
    )
    out_specs = (P("expert", "row", "col"), P("expert", "row"), P("expert", "col"))
    return jax.shard_map(body, mesh=mesh, in_specs=in_specs, out_specs=out_specs, check_vma=False)
```
